128 devices in a mesh: grp: 8 (over y, core), mem: 16 (over x, z).
Axes of the slice: x: 4, y: 4, z: 4, core: 2. Of those that a mesh axis runs over, the one named last changes fastest.
Arguments:
- factors: bfloat16 [256, 288, 1792], P(('grp', 'mem')), may hold values from -3 to 3
- screen: int32 [128, 18], P(('grp', 'mem')), may hold values from 0 to 1, as said below
Outputs:
- exchange_matrix: float32 [1792, 1792], P(('grp', 'mem'))
The draws below stay inside these ranges and needn't reach their ends.
Inputs may be any that keep to these rules, and one draw needn't show every extreme that they name: screen[b, j] is 1 where auxiliary block b and occupied block j survive screening; every auxiliary block keeps at least one occupied block.
All inputs are finite; a program needn't handle non-finite values.
Results may differ from the reference program's by a relative error of at most 0.0003.
Values may be sent and summed in bfloat16 or wider, within the bound.
No kernel may reach another device: no remote copies, remote signals or barrier semaphores. Data moves between devices by JAX's collectives and lax.ppermute only.
A program may use at most 128 MiB of HBM per device.

```python
import jax
import jax.numpy as jnp
from jax import lax

NBF = 1792
NOCC = 288
NOB = 18
NAB = 128
NAUX = 256


def draw_screen(key, part):
    count_key = jax.random.fold_in(key, 11)
    shuffle_key = jax.random.fold_in(key, 23)
    kept_count = jax.random.randint(count_key, (NAB, 1), 1, NOB + 1)
    row_keys = jax.random.split(shuffle_key, NAB)

    def shuffle_row(row_key):
        return jax.random.permutation(row_key, NOB)
    shuffled = jax.vmap(shuffle_row)(row_keys)
    position = jnp.argsort(shuffled, axis=1)
    return (position < kept_count).astype(jnp.int32)


def with_spikes(array, own_key, source, target, blocks, factor):
    def block_of(dim):
        return (jnp.arange(array.shape[dim]) // (array.shape[dim] // blocks)).reshape((-1,) + (1,) * (array.ndim - 1 - dim))

    near = jax.random.permutation(own_key, blocks)[block_of(target)]
    second = (block_of(target) + blocks // 2) % blocks
    return jnp.where((block_of(source) == near) | (block_of(source) == second), factor * array, array)


def steps_of(own_key, extent, pieces, low, top_value):
    def one(axis_at, parts):
        draws = jax.random.uniform(jax.random.fold_in(jax.random.fold_in(own_key, 6), axis_at), (parts,), jnp.float32, low / len(pieces), top_value / len(pieces))
        return jnp.repeat(jnp.exp(draws), extent[axis_at] // parts).reshape((-1,) + (1,) * (len(extent) - axis_at - 1))

    level = one(*pieces[0])
    for cut in pieces[1:]:
        level = level * one(*cut)
    return level


def bell_draw_with(own_key, dims, width, most, cuts, heavy, dtype=jnp.bfloat16):
    values = width * jax.random.normal(own_key, dims, jnp.float32)
    if cuts:
        values = values * steps_of(own_key, dims, cuts, -0.22, 0.18)
    return jnp.clip(with_spikes(values, jax.random.fold_in(own_key, 3), *heavy), -most, most).astype(dtype)


def setup_inputs(seed: int = 0) -> dict:
    keys = jax.random.split(jax.random.key(seed), 3)
    factors = bell_draw_with(keys[0], (NAUX, NOCC, NBF), 0.05, 3.0, ((0, 128),), (0, 2, 128, 5.5))
    screen = draw_screen(jax.random.fold_in(keys[2], 71), 0)
    return {"factors": factors, "screen": screen}


def reference(factors, screen):
    total_aux, occ_count, basis = factors.shape
    block_count, occ_blocks = screen.shape
    aux_rows = total_aux // block_count
    occ_width = occ_count // occ_blocks
    grouped = factors.reshape(block_count, aux_rows, occ_blocks, occ_width, basis)

    def add_block(running, pair):
        block, flags = pair
        masked = block * flags.astype(jnp.bfloat16)[None, :, None, None]
        flat_rows = masked.reshape(-1, basis)
        return running + jnp.dot(flat_rows.T, flat_rows, preferred_element_type=jnp.float32), None

    result, _ = lax.scan(add_block, jnp.zeros((basis, basis), jnp.float32), (grouped, screen))
    return result
```

```python
import functools

import jax
import jax.numpy as jnp
import numpy as np
from jax import lax
from jax.experimental import pallas as pl
from jax.experimental.pallas import tpu as pltpu
from jax.sharding import PartitionSpec as P


AXES = ("grp", "mem")
SIDE = 4
CORES = 2
WIDE_A = 1024
SENT = jnp.float16
LIMIT = pltpu.CompilerParams(vmem_limit_bytes=56 * 1024 * 1024)


def near(v):
    return v ^ 1


def far(v):
    return SIDE - 1 - v


def steps(core):
    return (near, far) if core == 0 else (far, near)


def order(v, core):
    first, second = steps(core)
    return [v, second(v), first(v), second(first(v))]


def linear(y, c, x, z):
    return ((y * CORES + c) * SIDE + x) * SIDE + z


def everyone():
    return [(y, c, x, z) for y in range(SIDE) for c in range(CORES) for x in range(SIDE) for z in range(SIDE)]


def partners(dim, turn):
    pairs = []
    for place in everyone():
        target = list(place)
        target[dim] = steps(place[1])[turn](place[dim])
        pairs.append((linear(*place), linear(*target)))
    return pairs


CORE_SWAP = [(linear(y, c, x, z), linear(y, 1 - c, x, z)) for y, c, x, z in everyone()]


def table():
    rows = []
    for y, c, x, z in everyone():
        x_order, z_order = order(x, c), order(z, c)
        row = [c, *order(y, c), *[x_order.index(v) for v in range(SIDE)], *[z_order.index(v) for v in range(SIDE)]]
        rows.append(row + [0] * (16 - len(row)))
    return np.asarray(rows, np.int32)


def transpose_kernel(where, screen, x_ref, out_ref, scratch):
    aux, occ, basis = x_ref.shape
    blocks = screen.shape[1]
    width = occ // blocks
    part = out_ref.shape[1]
    masked = []
    for a in range(aux):
        for b in range(blocks):
            flag = (screen[0, b] == 1).astype(jnp.float32)
            masked.append(x_ref[a, b * width : (b + 1) * width, :] * flag.astype(jnp.bfloat16))
    flat = jnp.concatenate(masked, axis=0)
    for t in range(basis // 128):
        scratch[t * 128 : (t + 1) * 128, :] = flat[:, t * 128 : (t + 1) * 128].T
    for s in range(SIDE):
        at = pl.multiple_of((where[1 + s] * CORES + where[0]) * part, 16)
        out_ref[s] = scratch[pl.ds(at, part), :]


def masked_transpose(where, screen, x):
    aux, occ, basis = x.shape
    part = basis // (SIDE * CORES)
    return pl.pallas_call(
        transpose_kernel,
        out_shape=jax.ShapeDtypeStruct((SIDE, part, aux * occ), x.dtype),
        in_specs=[pl.BlockSpec(memory_space=pltpu.SMEM)] * 2 + [pl.BlockSpec(memory_space=pltpu.VMEM)],
        out_specs=pl.BlockSpec(memory_space=pltpu.VMEM),
        scratch_shapes=[pltpu.VMEM((basis, aux * occ), x.dtype)],
        compiler_params=LIMIT,
    )(where, screen, x)


def product_kernel(slots, columns, where, own_t, other_t, own, other, *outs):
    deep = own_t.shape[2]
    part = own_t.shape[1]
    chunk = part // SIDE
    start, size = columns
    right = jnp.concatenate(
        [own[:, :, start : start + size].reshape(deep, size), other[:, :, start : start + size].reshape(deep, size)], axis=0
    )
    for at, s in enumerate(slots):
        left = jnp.concatenate([own_t[s], other_t[s]], axis=1)
        whole = jnp.dot(left, right, preferred_element_type=jnp.float32)
        for v in range(SIDE):
            piece = whole[v * chunk : (v + 1) * chunk]
            to = where[5 + v]
            if len(outs) == 1:
                outs[0][at, to] = piece
            else:
                for half, out in enumerate(outs):

                    @pl.when(to // 2 == half)
                    def _():
                        out[at, to % 2] = piece


def product(where, own_t, other_t, own, other, slots, columns, split):
    chunk = own_t.shape[1] // SIDE
    n = len(slots)
    if split:
        shapes = [jax.ShapeDtypeStruct((n, 2, chunk, columns[1]), jnp.float32)] * 2
    else:
        shapes = [jax.ShapeDtypeStruct((n, SIDE, chunk, columns[1]), jnp.float32)]
    rows = n * own_t.shape[1]
    depth = 2 * own_t.shape[2]
    return pl.pallas_call(
        functools.partial(product_kernel, slots, columns),
        out_shape=shapes,
        in_specs=[pl.BlockSpec(memory_space=pltpu.SMEM)] + [pl.BlockSpec(memory_space=pltpu.VMEM)] * 4,
        out_specs=[pl.BlockSpec(memory_space=pltpu.VMEM)] * len(shapes),
        compiler_params=LIMIT,
        cost_estimate=pl.CostEstimate(flops=2 * rows * depth * columns[1], bytes_accessed=4 * rows * columns[1], transcendentals=0),
    )(where, own_t, other_t, own, other)


def last_order_kernel(where, kept, arrived, keep_out, send_out, scratch):
    whole = kept[...] + arrived[...].astype(jnp.float32)
    rows = whole.shape[0] // SIDE
    for v in range(SIDE):
        scratch[where[9 + v]] = whole[v * rows : (v + 1) * rows]
    keep_out[...] = scratch[0:2]
    send_out[...] = scratch[2:4]


def last_order(where, kept, arrived):
    rows, basis = kept.shape
    half = jax.ShapeDtypeStruct((2, rows // SIDE, basis), jnp.float32)
    return pl.pallas_call(
        last_order_kernel,
        out_shape=[half, half],
        in_specs=[pl.BlockSpec(memory_space=pltpu.SMEM)] + [pl.BlockSpec(memory_space=pltpu.VMEM)] * 2,
        out_specs=[pl.BlockSpec(memory_space=pltpu.VMEM)] * 2,
        scratch_shapes=[pltpu.VMEM((SIDE, rows // SIDE, basis), jnp.float32)],
        compiler_params=LIMIT,
    )(where, kept, arrived)


def on_device(factors, screen):
    basis = factors.shape[2]
    f32 = jnp.float32
    where = lax.dynamic_index_in_dim(jnp.asarray(table()), lax.axis_index(AXES), 0, keepdims=False)
    other = lax.ppermute(factors, AXES, CORE_SWAP)
    other_screen = lax.ppermute(screen, AXES, CORE_SWAP)
    own_t = masked_transpose(where, screen, factors)
    other_t = masked_transpose(where, other_screen, other)
    left, right = (0, WIDE_A), (WIDE_A, basis - WIDE_A)

    def make(slots, columns, split):
        return product(where, own_t, other_t, factors, other, slots, columns, split)

    def narrow(v):
        return v.astype(SENT)

    def go(v, dim, turn):
        return lax.ppermute(v, AXES, partners(dim, turn))

    (a_send,) = make((2, 3), left, False)
    a_in = go(narrow(a_send), 0, 0)
    b_keep, b_send = make((0, 1, 2, 3), right, True)
    b_in = go(narrow(b_send), 2, 0)
    (a_keep,) = make((0, 1), left, False)
    a_in2 = go(narrow(a_keep[:, 2:] + a_in[:, 2:].astype(f32)), 2, 0)
    a_keep = a_keep[:, :2] + a_in[:, :2].astype(f32)
    b_in2 = go(narrow(b_keep[2:] + b_in[2:].astype(f32)), 0, 0)
    b_keep = b_keep[:2] + b_in[:2].astype(f32)

    def joined(slot):
        return jnp.concatenate(
            [a_keep[slot] + a_in2[slot].astype(f32), b_keep[slot] + b_in2[slot].astype(f32)], axis=-1
        )

    c_in = go(narrow(joined(1)), 0, 1)
    c_keep = joined(0)
    d_in = go(narrow(c_keep[1] + c_in[1].astype(f32)), 2, 1)
    d_keep = c_keep[0] + c_in[0].astype(f32)
    e_keep, e_send = last_order(where, d_keep, d_in.astype(f32))
    e_in = go(e_send, 3, 0)
    f_in = go(e_keep[1] + e_in[1], 3, 1)
    return e_keep[0] + e_in[0] + f_in


def solution(mesh):
    placed = (P(AXES, None, None), P(AXES, None))
    return jax.shard_map(on_device, mesh=mesh, in_specs=placed, out_specs=P(AXES, None), check_vma=False)
```

```python
import functools

import jax
import jax.numpy as jnp
import numpy as np
from jax import lax
from jax.experimental import pallas as pl
from jax.experimental.pallas import tpu as pltpu
from jax.sharding import PartitionSpec as P


AXES = ("grp", "mem")
SIDE = 4
CORES = 2
WIDE_A = 1152
SENT = jnp.float16


def limit(mib):
    return pltpu.CompilerParams(vmem_limit_bytes=mib * 1024 * 1024)


def near(v):
    return v ^ 1


def far(v):
    return SIDE - 1 - v


def steps(dim, core):
    return (near, far) if core == (dim == 2) else (far, near)


def order(v, dim, core):
    first, second = steps(dim, core)
    return [v, second(v), first(v), second(first(v))]


def linear(y, c, x, z):
    return ((y * CORES + c) * SIDE + x) * SIDE + z


def everyone():
    return [(y, c, x, z) for y in range(SIDE) for c in range(CORES) for x in range(SIDE) for z in range(SIDE)]


def partners(*moves):
    pairs = []
    for place in everyone():
        target = list(place)
        for dim, turn in moves:
            target[dim] = steps(dim, place[1])[turn](target[dim])
        pairs.append((linear(*place), linear(*target)))
    return pairs


CORE_SWAP = [(linear(y, c, x, z), linear(y, 1 - c, x, z)) for y, c, x, z in everyone()]


def table():
    rows = []
    for y, c, x, z in everyone():
        x_order, z_order = order(x, 2, c), order(z, 3, c)
        row = [c, *order(y, 0, c), *[x_order.index(v) for v in range(SIDE)], *[z_order.index(v) for v in range(SIDE)]]
        rows.append(row + [0] * (16 - len(row)))
    return np.asarray(rows, np.int32)


def transpose_kernel(where, x_ref, out_ref, same_ref, scratch):
    aux, occ, basis = x_ref.shape
    part = out_ref.shape[1]
    same_ref[...] = x_ref[...]
    for a in range(aux):
        for t in range(basis // 128):
            scratch[t * 128 : (t + 1) * 128, a * occ : (a + 1) * occ] = x_ref[a, :, t * 128 : (t + 1) * 128].T
    for s in range(SIDE):
        at = pl.multiple_of((where[1 + s] * CORES + where[0]) * part, 16)
        out_ref[s] = scratch[pl.ds(at, part), :]


def transposed(where, x):
    aux, occ, basis = x.shape
    part = basis // (SIDE * CORES)
    return pl.pallas_call(
        transpose_kernel,
        out_shape=[jax.ShapeDtypeStruct((SIDE, part, aux * occ), x.dtype), jax.ShapeDtypeStruct(x.shape, x.dtype)],
        in_specs=[pl.BlockSpec(memory_space=pltpu.SMEM)] + [pl.BlockSpec(memory_space=pltpu.VMEM)],
        out_specs=[pl.BlockSpec(memory_space=pltpu.VMEM)] * 2,
        scratch_shapes=[pltpu.VMEM((basis, aux * occ), x.dtype)],
        compiler_params=limit(12),
    )(where, x)


def product_kernel(slots, columns, where, flags, own_t, other_t, own, other, out):
    deep = own_t.shape[2]
    part = own_t.shape[1]
    chunk = part // SIDE
    start, size = columns
    right = jnp.concatenate(
        [own[:, :, start : start + size].reshape(deep, size), other[:, :, start : start + size].reshape(deep, size)], axis=0
    )
    for at, s in enumerate(slots):
        left = jnp.concatenate([own_t[s], other_t[s]], axis=1) * flags[...]
        whole = jnp.dot(left, right, preferred_element_type=jnp.float32)
        for v in range(SIDE):
            out[at, where[5 + v]] = whole[v * chunk : (v + 1) * chunk]


def product(where, flags, own_t, other_t, own, other, slots, columns):
    chunk = own_t.shape[1] // SIDE
    n = len(slots)
    rows = n * own_t.shape[1]
    depth = 2 * own_t.shape[2]
    vmem = pl.BlockSpec(memory_space=pltpu.VMEM)
    return pl.pallas_call(
        functools.partial(product_kernel, slots, columns),
        out_shape=jax.ShapeDtypeStruct((n, SIDE, chunk, columns[1]), jnp.float32),
        in_specs=[pl.BlockSpec(memory_space=pltpu.SMEM)] + [vmem] * 5,
        out_specs=vmem,
        compiler_params=limit(16),
        cost_estimate=pl.CostEstimate(flops=2 * rows * depth * columns[1], bytes_accessed=4 * rows * columns[1], transcendentals=0),
    )(where, flags, own_t, other_t, own, other)


def last_order_kernel(where, whole_ref, *refs):
    outs, scratch = refs[:-1], refs[-1]
    whole = whole_ref[...]
    rows = whole.shape[0] // SIDE
    for v in range(SIDE):
        scratch[where[9 + v]] = whole[v * rows : (v + 1) * rows]
    for slot, out in enumerate(outs):
        out[...] = scratch[slot]


def last_order(where, whole):
    rows, basis = whole.shape
    part = jax.ShapeDtypeStruct((rows // SIDE, basis), jnp.float32)
    return pl.pallas_call(
        last_order_kernel,
        out_shape=[part] * SIDE,
        in_specs=[pl.BlockSpec(memory_space=pltpu.SMEM), pl.BlockSpec(memory_space=pltpu.VMEM)],
        out_specs=[pl.BlockSpec(memory_space=pltpu.VMEM)] * SIDE,
        scratch_shapes=[pltpu.VMEM((SIDE, rows // SIDE, basis), jnp.float32)],
        compiler_params=limit(4),
    )(where, whole)


def on_device(factors, screen):
    basis = factors.shape[2]
    f32 = jnp.float32
    where = lax.dynamic_index_in_dim(jnp.asarray(table()), lax.axis_index(AXES), 0, keepdims=False)
    other = lax.ppermute(factors, AXES, CORE_SWAP)
    other_screen = lax.ppermute(screen, AXES, CORE_SWAP)
    own_t, own = transposed(where, factors)
    other_t, other = transposed(where, other)
    both = jnp.concatenate([screen, other_screen], axis=0) == 1
    width = factors.shape[1] // screen.shape[1]
    flags = jnp.broadcast_to(both.astype(jnp.bfloat16)[:, None, :, None], (2, factors.shape[0], screen.shape[1], width))
    flags = flags.reshape(1, -1)
    left, right = (0, WIDE_A), (WIDE_A, basis - WIDE_A)

    def make(slots, columns):
        return product(where, flags, own_t, other_t, own, other, slots, columns)

    def narrow(v):
        return v.astype(SENT)

    def go(v, *moves):
        return lax.ppermute(v, AXES, partners(*moves))

    a_send = make((2, 3), left)
    a_in = go(narrow(a_send), (0, 0))
    b_all = make((0, 1, 2, 3), right)
    b_in = go(narrow(b_all[:, 2:]), (2, 0))
    a_keep = make((0, 1), left)
    a_in2 = go(narrow(a_keep[:, 2:] + a_in[:, 2:].astype(f32)), (2, 0))
    a_keep = a_keep[:, :2] + a_in[:, :2].astype(f32)
    b_in2 = go(narrow(b_all[2:, :2] + b_in[2:].astype(f32)), (0, 0))
    b_keep = b_all[:2, :2] + b_in[:2].astype(f32)

    def joined(i, j):
        return jnp.concatenate(
            [a_keep[i, j] + a_in2[i, j].astype(f32), b_keep[i, j] + b_in2[i, j].astype(f32)], axis=-1
        )

    c_y = go(narrow(joined(1, 0)), (0, 1))
    c_x = go(narrow(joined(0, 1)), (2, 1))
    c_d = go(narrow(joined(1, 1)), (0, 1), (2, 1))
    whole = joined(0, 0) + c_y.astype(f32) + c_x.astype(f32) + c_d.astype(f32)
    kept, second, first, across = last_order(where, whole)
    d_first = go(first, (3, 0))
    d_second = go(second, (3, 1))
    d_across = go(across, (3, 0), (3, 1))
    return kept + d_second + d_first + d_across


def solution(mesh):
    placed = (P(AXES, None, None), P(AXES, None))
    return jax.shard_map(on_device, mesh=mesh, in_specs=placed, out_specs=P(AXES, None), check_vma=False)
```

```python
import functools

import jax
import jax.numpy as jnp
import numpy as np
from jax import lax
from jax.experimental import pallas as pl
from jax.experimental.pallas import tpu as pltpu
from jax.sharding import PartitionSpec as P


AXES = ("grp", "mem")
SIDE = 4
CORES = 2
STRIPE = 256
SENT = jnp.float16
F32 = jnp.float32


def limit(mib):
    return pltpu.CompilerParams(vmem_limit_bytes=mib * 1024 * 1024)


VMEM = pl.BlockSpec(memory_space=pltpu.VMEM)
SMEM = pl.BlockSpec(memory_space=pltpu.SMEM)
HBM = pl.BlockSpec(memory_space=pltpu.HBM)


def near(v):
    return v ^ 1


def far(v):
    return SIDE - 1 - v


def steps(dim, core):
    return (near, far) if core == (dim == 2) else (far, near)


def order(v, dim, core):
    first, second = steps(dim, core)
    return [v, second(v), first(v), second(first(v))]


def linear(y, c, x, z):
    return ((y * CORES + c) * SIDE + x) * SIDE + z


def everyone():
    return [(y, c, x, z) for y in range(SIDE) for c in range(CORES) for x in range(SIDE) for z in range(SIDE)]


def partners(*moves):
    pairs = []
    for place in everyone():
        target = list(place)
        for dim, turn in moves:
            target[dim] = steps(dim, place[1])[turn](target[dim])
        pairs.append((linear(*place), linear(*target)))
    return pairs


CORE_SWAP = [(linear(y, c, x, z), linear(y, 1 - c, x, z)) for y, c, x, z in everyone()]


def table():
    rows = []
    for y, c, x, z in everyone():
        z_order = order(z, 3, c)
        row = [c, *order(y, 0, c), *order(x, 2, c), *[z_order.index(v) for v in range(SIDE)]]
        rows.append(row + [0] * (16 - len(row)))
    return np.asarray(rows, np.int32)


def padded(depth):
    return -(-depth // 128) * 128


def front_kernel(base, where, flags, x_ref, *refs):
    x_all, x_t, scratch, sems = refs[-4:]
    before = refs[:-4]
    aux, occ, basis = x_ref.shape
    depth = aux * occ
    part = basis // (SIDE * CORES)
    chunk = part // SIDE
    pad = padded(depth) - depth
    copies = []
    for j in range(basis // STRIPE):
        columns = slice(j * STRIPE, (j + 1) * STRIPE)
        pair = [
            pltpu.make_async_copy(
                x_ref.at[a, :, columns], x_all.at[pl.ds(base + a * occ, occ), columns], sems.at[j, a]
            )
            for a in range(aux)
        ]
        for copy in pair:
            copy.start()
        copies.append(pair)
    if before:
        x_all[:base, :] = before[0][...]
        x_t[:, :, :, :base] = before[1][...]
    x_all[base + depth : base + depth + pad, :] = jnp.zeros((pad, basis), x_all.dtype)
    for j, pair in enumerate(copies):
        for copy in pair:
            copy.wait()
        columns = slice(j * STRIPE, (j + 1) * STRIPE)
        scratch[columns, :] = x_all[base : base + depth, columns].T
    for s in range(SIDE):
        at = pl.multiple_of((where[1 + s] * CORES + where[0]) * part, 16)
        block = scratch[pl.ds(at, part), :] * flags[...]
        block = jnp.concatenate([block, jnp.zeros((part, pad), block.dtype)], axis=1)
        for v in range(SIDE):
            x_t[s, v, :, base : base + depth + pad] = block[v * chunk : (v + 1) * chunk]


def front(where, flags, x, before):
    aux, occ, basis = x.shape
    depth = aux * occ
    chunk = basis // (SIDE * CORES * SIDE)
    base = padded(depth) if before else 0
    full = base + padded(depth)
    return pl.pallas_call(
        functools.partial(front_kernel, base),
        out_shape=[
            jax.ShapeDtypeStruct((full, basis), x.dtype),
            jax.ShapeDtypeStruct((SIDE, SIDE, chunk, full), x.dtype),
        ],
        in_specs=[SMEM, VMEM, HBM] + [VMEM] * len(before),
        out_specs=[VMEM] * 2,
        scratch_shapes=[pltpu.VMEM((basis, depth), x.dtype), pltpu.SemaphoreType.DMA((basis // STRIPE, aux))],
        compiler_params=limit(16),
    )(where, flags, x, *before)


def product_kernel(slots, where, x_all, x_t, out):
    chunk = x_t.shape[2]
    left = jnp.concatenate([x_t[i, where[5 + j]] for i, j in slots], axis=0)
    whole = jnp.dot(left, x_all[...], preferred_element_type=F32)
    for at in range(len(slots)):
        out[at] = whole[at * chunk : (at + 1) * chunk]


def product(where, x_all, x_t, slots):
    chunk, depth = x_t.shape[2:]
    basis = x_all.shape[1]
    rows = len(slots) * chunk
    return pl.pallas_call(
        functools.partial(product_kernel, slots),
        out_shape=jax.ShapeDtypeStruct((len(slots), chunk, basis), F32),
        in_specs=[SMEM, VMEM, VMEM],
        out_specs=VMEM,
        compiler_params=limit(16),
        cost_estimate=pl.CostEstimate(flops=2 * rows * depth * basis, bytes_accessed=4 * rows * basis, transcendentals=0),
    )(where, x_all, x_t)


def last_order_kernel(where, whole_ref, *refs):
    outs, scratch = refs[:-1], refs[-1]
    whole = whole_ref[...]
    rows = whole.shape[0] // SIDE
    for v in range(SIDE):
        scratch[where[9 + v]] = whole[v * rows : (v + 1) * rows]
    for slot, out in enumerate(outs):
        out[...] = scratch[slot]


def last_order(where, whole):
    rows, basis = whole.shape
    part = jax.ShapeDtypeStruct((rows // SIDE, basis), F32)
    return pl.pallas_call(
        last_order_kernel,
        out_shape=[part] * SIDE,
        in_specs=[SMEM, VMEM],
        out_specs=[VMEM] * SIDE,
        scratch_shapes=[pltpu.VMEM((SIDE, rows // SIDE, basis), F32)],
        compiler_params=limit(4),
    )(where, whole)


def go(v, *moves):
    return lax.ppermute(v, AXES, partners(*moves))


def narrow(v):
    return v.astype(SENT)


def wide(v):
    return v.astype(F32)


def on_device(factors, screen):
    where = lax.dynamic_index_in_dim(jnp.asarray(table()), lax.axis_index(AXES), 0, keepdims=False)
    other = lax.ppermute(factors, AXES, CORE_SWAP)
    other_screen = lax.ppermute(screen, AXES, CORE_SWAP)
    aux, occ, _ = factors.shape
    blocks = screen.shape[1]

    def flags_of(mask):
        kept = (mask == 1).astype(factors.dtype)
        return jnp.broadcast_to(kept[:, :, None], (aux, blocks, occ // blocks)).reshape(1, aux * occ)

    held = front(where, flags_of(screen), factors, ())
    x_all, x_t = front(where, flags_of(other_screen), other, held)

    def make(*slots):
        return product(where, x_all, x_t, slots)

    y_first, x_first, y_second, x_second = (0, 0), (2, 0), (0, 1), (2, 1)
    d_out = make((2, 2), (2, 3), (3, 2), (3, 3))
    d_in = go(narrow(d_out), y_first, x_first)
    y_out = make((2, 0), (2, 1), (3, 0), (3, 1))
    y_in = go(narrow(y_out), y_first)
    x_out = make((0, 2), (0, 3), (1, 2), (1, 3))
    x_in = go(narrow(x_out), x_first)
    kept = make((0, 0), (0, 1), (1, 0), (1, 1))

    def added(i):
        return kept[i] + wide(d_in[i]) + wide(y_in[i]) + wide(x_in[i])

    d_in2 = go(narrow(added(3)), y_second, x_second)
    y_in2 = go(narrow(added(2)), y_second)
    x_in2 = go(narrow(added(1)), x_second)
    whole = added(0) + wide(d_in2) + wide(y_in2) + wide(x_in2)
    kept, second, first, across = last_order(where, whole)
    z_across = go(across, (3, 0), (3, 1))
    z_second = go(second, (3, 1))
    z_first = go(first, (3, 0))
    return kept + z_second + z_first + z_across


def solution(mesh):
    placed = (P(AXES, None, None), P(AXES, None))
    return jax.shard_map(on_device, mesh=mesh, in_specs=placed, out_specs=P(AXES, None), check_vma=False)
```

```python
import functools

import jax
import jax.numpy as jnp
from jax import lax
from jax.experimental import pallas as pl
from jax.experimental.pallas import tpu as pltpu
from jax.sharding import PartitionSpec as P


AXES = ("grp", "mem")
SIDE = 4
CORES = 2
STRIPE = 256
SENT = jnp.float16
ROOM = 16384.0
SMALLEST = 2.0**-60
F32 = jnp.float32


def limit(mib):
    return pltpu.CompilerParams(vmem_limit_bytes=mib * 1024 * 1024)


VMEM = pl.BlockSpec(memory_space=pltpu.VMEM)
SMEM = pl.BlockSpec(memory_space=pltpu.SMEM)
HBM = pl.BlockSpec(memory_space=pltpu.HBM)


def near(v):
    return v ^ 1


def far(v):
    return SIDE - 1 - v


def steps(dim, core):
    return (near, far) if core == (dim == 2) else (far, near)


def linear(y, c, x, z):
    return ((y * CORES + c) * SIDE + x) * SIDE + z


def everyone():
    return [(y, c, x, z) for y in range(SIDE) for c in range(CORES) for x in range(SIDE) for z in range(SIDE)]


def partners(*moves):
    pairs = []
    for place in everyone():
        target = list(place)
        for dim, turn in moves:
            target[dim] = steps(dim, place[1])[turn](target[dim])
        pairs.append((linear(*place), linear(*target)))
    return pairs


CORE_SWAP = [(linear(y, c, x, z), linear(y, 1 - c, x, z)) for y, c, x, z in everyone()]


def here():
    group, member = lax.axis_index("grp"), lax.axis_index("mem")
    return lax.div(group, CORES), lax.rem(group, CORES), lax.div(member, SIDE), lax.rem(member, SIDE)


def order_here(v, dim, core):
    near_first = core == int(dim == 2)
    close, distant = v ^ 1, SIDE - 1 - v
    first, second = jnp.where(near_first, close, distant), jnp.where(near_first, distant, close)
    return [v, second, first, v ^ 2]


def bound(most, terms):
    return terms * most * most


def front_kernel(track, screen, x_ref, *refs):
    scratch, sems = refs[-2:]
    if track:
        x_out, x_t, *tail = refs[:-2]
    else:
        x_out, x_t = refs[2:4]
        tail = (*refs[:2], *refs[4:-2])
    y, core, _, _ = here()
    aux, occ, basis = x_ref.shape
    depth = aux * occ
    blocks = screen.shape[1]
    part = basis // (SIDE * CORES)
    chunk = part // SIDE
    copies = []
    for j in range(basis // STRIPE):
        columns = slice(j * STRIPE, (j + 1) * STRIPE)
        pair = [
            pltpu.make_async_copy(x_ref.at[a, :, columns], x_out.at[pl.ds(a * occ, occ), columns], sems.at[j, a])
            for a in range(aux)
        ]
        for copy in pair:
            copy.start()
        copies.append(pair)
    lane = lax.broadcasted_iota(jnp.int32, (16, depth), 1)
    block_of = lax.div(lax.rem(lane, occ), occ // blocks)
    flags = jnp.zeros((16, depth), F32)
    for b in range(blocks):
        flags = jnp.where(block_of == b, (screen[0, b] == 1).astype(F32), flags)
    flags = flags.astype(x_out.dtype)
    most = jnp.zeros((16, depth), x_out.dtype)
    for j, pair in enumerate(copies):
        for copy in pair:
            copy.wait()
        columns = slice(j * STRIPE, (j + 1) * STRIPE)
        turned = x_out[:, columns].T
        scratch[columns, :] = turned
        if track:
            sizes = jnp.abs(turned)
            for r in range(0, STRIPE, 16):
                most = jnp.maximum(most, sizes[r : r + 16])
    if track:
        most = (most * flags).astype(F32)
        top = jnp.max(jnp.max(most, axis=1, keepdims=True), axis=0, keepdims=True)
        tail[0][...] = jnp.broadcast_to(top, tail[0].shape)
    else:
        top = jnp.maximum(jnp.maximum(tail[0][...], tail[1][...]), SMALLEST)
        tail[2][...] = top
    for s, at in enumerate(order_here(y, 0, core)):
        first = pl.multiple_of((at * CORES + core) * part, 16)
        block = scratch[pl.ds(first, part), :] * flags[0:1]
        for v in range(SIDE):
            x_t[s, v] = block[v * chunk : (v + 1) * chunk]


def front(screen, x, peaks):
    aux, occ, basis = x.shape
    depth = aux * occ
    shapes = [
        jax.ShapeDtypeStruct((depth, basis), x.dtype),
        jax.ShapeDtypeStruct((SIDE, SIDE, basis // (SIDE * CORES * SIDE), depth), x.dtype),
        jax.ShapeDtypeStruct((8, 128), F32),
    ]
    return pl.pallas_call(
        functools.partial(front_kernel, not peaks),
        out_shape=shapes,
        in_specs=[SMEM, HBM] + [VMEM] * len(peaks),
        out_specs=[VMEM] * len(shapes),
        scratch_shapes=[pltpu.VMEM((basis, depth), x.dtype), pltpu.SemaphoreType.DMA((basis // STRIPE, aux))],
        compiler_params=limit(16),
    )(screen, x, *peaks)


def product_kernel(slots, x_own, t_own, x_other, t_other, *refs):
    out = refs[-1]
    _, core, x, _ = here()
    x_order = order_here(x, 2, core)
    chunk = t_own.shape[2]

    def left(x_t):
        return jnp.concatenate([x_t[i, x_order[j]] for i, j in slots], axis=0)

    whole = jnp.dot(left(t_own), x_own[...], preferred_element_type=F32)
    whole = whole + jnp.dot(left(t_other), x_other[...], preferred_element_type=F32)
    if len(refs) > 1:
        whole = whole * (ROOM / bound(refs[0][0:1, 0:1], CORES * x_own.shape[0]))
    for at in range(len(slots)):
        out[at] = whole[at * chunk : (at + 1) * chunk]


def product(parts, slots):
    chunk, depth = parts[1].shape[2:]
    basis = parts[0].shape[1]
    rows = len(slots) * chunk
    return pl.pallas_call(
        functools.partial(product_kernel, slots),
        out_shape=jax.ShapeDtypeStruct((len(slots), chunk, basis), F32),
        in_specs=[VMEM] * len(parts),
        out_specs=VMEM,
        compiler_params=limit(16),
        cost_estimate=pl.CostEstimate(flops=4 * rows * depth * basis, bytes_accessed=4 * rows * basis, transcendentals=0),
    )(*parts)


def power(e):
    return jnp.exp2(e).astype(jnp.bfloat16).astype(F32)


def settle_kernel(terms, kept, *refs):
    arrived, tiles, outs = refs[:3], refs[3:7], refs[7:]
    most = tiles[0][0:1, 0:1]
    rates = []
    for tile in tiles[1:]:
        most = jnp.maximum(most, tile[0:1, 0:1])
        rates.append(bound(tile[0:1, 0:1], terms) / ROOM)
    quarter = jnp.ceil(jnp.log2(bound(most, SIDE * terms) / ROOM) * 0.25)
    one = jnp.floor(quarter / 3)
    two = jnp.floor((quarter - one) / 2)
    scale = power(-4 * quarter)
    rows, basis = kept.shape[1:]
    for slot, out in enumerate(outs):
        whole = kept[slot]
        for block, rate in zip(arrived, rates):
            whole = whole + block[slot] * rate
        out[:rows] = whole * scale if slot else whole
        if slot:
            at = lax.broadcasted_iota(jnp.int32, (8, basis), 0)
            third = quarter - one - two
            out[rows : rows + 8] = power(jnp.where(at == 0, one, jnp.where(at == 1, two, third)))


def settle(terms, kept, arrived, tiles):
    rows, basis = kept.shape[1:]
    shapes = [jax.ShapeDtypeStruct((rows, basis), F32)]
    shapes += [jax.ShapeDtypeStruct((rows + 8, basis), F32)] * (SIDE - 1)
    return pl.pallas_call(
        functools.partial(settle_kernel, terms),
        out_shape=shapes,
        in_specs=[VMEM] * 8,
        out_specs=[VMEM] * SIDE,
        compiler_params=limit(8),
    )(kept, *arrived, *tiles)


def last_kernel(kept, *refs):
    arrived, outs, scratch = refs[:3], refs[3:-1], refs[-1]
    _, core, _, z = here()
    whole = kept[...]
    high = whole.shape[0]
    for block in arrived:
        rate = block[high : high + 1, 0:1] * block[high + 1 : high + 2, 0:1] * block[high + 2 : high + 3, 0:1]
        rate = rate * rate
        whole = whole + block[:high] * (rate * rate)
    rows = high // SIDE
    for v in range(SIDE):
        scratch[v] = whole[v * rows : (v + 1) * rows]
    for slot, out in zip(order_here(z, 3, core), outs):
        out[...] = scratch[slot]


def last(kept, arrived):
    rows, basis = kept.shape
    part = jax.ShapeDtypeStruct((rows // SIDE, basis), F32)
    return pl.pallas_call(
        last_kernel,
        out_shape=[part] * SIDE,
        in_specs=[VMEM] * 4,
        out_specs=[VMEM] * SIDE,
        scratch_shapes=[pltpu.VMEM((SIDE, rows // SIDE, basis), F32)],
        compiler_params=limit(4),
    )(kept, *arrived)


def go(v, *moves):
    return lax.ppermute(v, AXES, partners(*moves))


def on_device(factors, screen):
    other = lax.ppermute(factors, AXES, CORE_SWAP)
    other_screen = lax.ppermute(screen, AXES, CORE_SWAP)
    depth = CORES * factors.shape[0] * factors.shape[1]

    x_own, t_own, peak = front(screen, factors, ())
    x_other, t_other, peak = front(other_screen, other, (peak, lax.ppermute(peak, AXES, CORE_SWAP)))
    parts = (x_own, t_own, x_other, t_other)

    def narrow(v):
        return v.astype(SENT)

    def wide(v):
        return v.astype(F32)

    d_moves, y_moves, x_moves = ((0, 0), (2, 0)), ((0, 0),), ((2, 0),)
    d_out = product((*parts, peak), ((2, 2), (2, 3), (3, 2), (3, 3)))
    d_in = go(narrow(d_out), *d_moves)
    y_out = product((*parts, peak), ((2, 0), (2, 1), (3, 0), (3, 1)))
    y_in = go(narrow(y_out), *y_moves)
    x_out = product((*parts, peak), ((0, 2), (0, 3), (1, 2), (1, 3)))
    x_in = go(narrow(x_out), *x_moves)
    kept = product(parts, ((0, 0), (0, 1), (1, 0), (1, 1)))
    d_most = go(peak, *d_moves)
    y_most = go(peak, *y_moves)
    x_most = go(peak, *x_moves)
    kept, x_out, y_out, d_out = settle(
        depth, kept, (wide(d_in), wide(y_in), wide(x_in)), (peak, d_most, y_most, x_most)
    )

    d_moves, y_moves, x_moves = ((0, 1), (2, 1)), ((0, 1),), ((2, 1),)
    d_in = go(narrow(d_out), *d_moves)
    y_in = go(narrow(y_out), *y_moves)
    x_in = go(narrow(x_out), *x_moves)
    kept, second, first, across = last(kept, (wide(d_in), wide(y_in), wide(x_in)))
    z_across = go(across, (3, 0), (3, 1))
    z_second = go(second, (3, 1))
    z_first = go(first, (3, 0))
    return kept + z_second + z_first + z_across


def solution(mesh):
    placed = (P(AXES, None, None), P(AXES, None))
    return jax.shard_map(on_device, mesh=mesh, in_specs=placed, out_specs=P(AXES, None), check_vma=False)
```

```python
import functools

import jax
import jax.numpy as jnp
from jax import lax
from jax.experimental import pallas as pl
from jax.experimental.pallas import tpu as pltpu
from jax.sharding import PartitionSpec as P


AXES = ("grp", "mem")
SIDE = 4
CORES = 2
SENT = jnp.float16
ROOM = 16384.0
SMALLEST = 2.0**-60
F32 = jnp.float32


def limit(mib):
    return pltpu.CompilerParams(vmem_limit_bytes=mib * 1024 * 1024)


VMEM = pl.BlockSpec(memory_space=pltpu.VMEM)
SMEM = pl.BlockSpec(memory_space=pltpu.SMEM)


def near(v):
    return v ^ 1


def far(v):
    return SIDE - 1 - v


def steps(dim, core):
    return (near, far) if core == (dim == 2) else (far, near)


def linear(y, c, x, z):
    return ((y * CORES + c) * SIDE + x) * SIDE + z


def everyone():
    return [(y, c, x, z) for y in range(SIDE) for c in range(CORES) for x in range(SIDE) for z in range(SIDE)]


def partners(*moves):
    pairs = []
    for place in everyone():
        target = list(place)
        for dim, turn in moves:
            target[dim] = steps(dim, place[1])[turn](target[dim])
        pairs.append((linear(*place), linear(*target)))
    return pairs


CORE_SWAP = [(linear(y, c, x, z), linear(y, 1 - c, x, z)) for y, c, x, z in everyone()]


def here():
    group, member = lax.axis_index("grp"), lax.axis_index("mem")
    return lax.div(group, CORES), lax.rem(group, CORES), lax.div(member, SIDE), lax.rem(member, SIDE)


def order_here(v, dim, core):
    near_first = core == int(dim == 2)
    close, distant = v ^ 1, SIDE - 1 - v
    first, second = jnp.where(near_first, close, distant), jnp.where(near_first, distant, close)
    return [v, second, first, v ^ 2]


def bound(most, terms):
    return terms * most * most


def padded(size, tile):
    return -(-size // tile) * tile


def front_kernel(slots, aux, screen, x_ref, *refs):
    outs, scratch = refs[:-1], refs[-1]
    y, core, _, _ = here()
    depth, basis = x_ref.shape
    blocks = screen.shape[1]
    part = basis // (SIDE * CORES)
    chunk = part // SIDE
    span = scratch.shape[1]
    occ = depth // aux
    lane = lax.broadcasted_iota(jnp.int32, (16, depth), 1)
    block_of = lax.div(lax.rem(lane, occ), occ // blocks)
    flags = jnp.zeros((16, depth), F32)
    for b in range(blocks):
        flags = jnp.where(block_of == b, (screen[0, b] == 1).astype(F32), flags)
    flags = flags.astype(x_ref.dtype)
    if len(outs) > len(slots):
        width = occ // blocks
        most = jnp.zeros((width, basis), F32)
        for r in range(0, depth, width):
            kept = (screen[0, (r % occ) // width] == 1).astype(F32)
            most = jnp.maximum(most, jnp.abs(x_ref[r : r + width, :]).astype(F32) * kept)
        top = jnp.max(jnp.max(most, axis=1, keepdims=True), axis=0, keepdims=True)
        outs[-1][...] = jnp.broadcast_to(top, outs[-1].shape)
    places = order_here(y, 0, core)
    for n, pair in enumerate(slots):
        for s, slot in enumerate(pair):
            start = (places[slot] * CORES + core) * part
            tile = jnp.minimum(lax.div(start, 128), (basis - span) // 128)
            held = scratch.at[(2 * n + s) % 2]
            held[...] = x_ref[:, pl.ds(pl.multiple_of(tile * 128, 128), span)].T
            block = held[pl.ds(pl.multiple_of(start - tile * 128, 16), part), :] * flags[0:1]
            for v in range(SIDE):
                outs[n][s, v] = block[v * chunk : (v + 1) * chunk]


def front(screen, x, aux, slots, peak):
    depth, basis = x.shape
    part = basis // (SIDE * CORES)
    span = padded(part + 127, 128)
    shapes = [jax.ShapeDtypeStruct((2, SIDE, part // SIDE, depth), x.dtype)] * len(slots)
    if peak:
        shapes.append(jax.ShapeDtypeStruct((8, 128), F32))
    return pl.pallas_call(
        functools.partial(front_kernel, slots, aux),
        out_shape=shapes,
        in_specs=[SMEM, VMEM],
        out_specs=[VMEM] * len(shapes),
        scratch_shapes=[pltpu.VMEM((2, span, depth), x.dtype)],
        compiler_params=limit(12),
    )(screen, x)


def bound(most, terms):
    return terms * most * most


def product_kernel(slots, x_own, t_own, x_other, t_other, *refs):
    out = refs[-1]
    _, core, x, _ = here()
    x_order = order_here(x, 2, core)
    chunk = t_own.shape[2]

    def left(x_t):
        return jnp.concatenate([x_t[i, x_order[j]] for i, j in slots], axis=0)

    whole = jnp.dot(left(t_own), x_own[...], preferred_element_type=F32)
    whole = whole + jnp.dot(left(t_other), x_other[...], preferred_element_type=F32)
    if len(refs) > 1:
        most = jnp.maximum(jnp.maximum(refs[0][0:1, 0:1], refs[1][0:1, 0:1]), SMALLEST)
        whole = whole * (ROOM / bound(most, CORES * x_own.shape[0]))
    for at in range(len(slots)):
        out[at] = whole[at * chunk : (at + 1) * chunk]


def product(parts, slots):
    chunk, depth = parts[1].shape[2:]
    basis = parts[0].shape[1]
    rows = len(slots) * chunk
    return pl.pallas_call(
        functools.partial(product_kernel, slots),
        out_shape=jax.ShapeDtypeStruct((len(slots), chunk, basis), F32),
        in_specs=[VMEM] * len(parts),
        out_specs=VMEM,
        compiler_params=limit(16),
        cost_estimate=pl.CostEstimate(flops=4 * rows * depth * basis, bytes_accessed=4 * rows * basis, transcendentals=0),
    )(*parts)


def power(e):
    return jnp.exp2(e).astype(jnp.bfloat16).astype(F32)


def settle_kernel(terms, kept, *refs):
    arrived, tiles, outs = refs[:3], refs[3:7], refs[7:]
    most = tiles[0][0:1, 0:1]
    rates = []
    for tile in tiles[1:]:
        most = jnp.maximum(most, tile[0:1, 0:1])
        rates.append(bound(tile[0:1, 0:1], terms) / ROOM)
    quarter = jnp.ceil(jnp.log2(bound(most, SIDE * terms) / ROOM) * 0.25)
    one = jnp.floor(quarter / 3)
    two = jnp.floor((quarter - one) / 2)
    scale = power(-4 * quarter)
    rows, basis = kept.shape[1:]
    for slot, out in enumerate(outs):
        whole = kept[slot]
        for block, rate in zip(arrived, rates):
            whole = whole + block[slot] * rate
        out[:rows] = whole * scale if slot else whole
        if slot:
            at = lax.broadcasted_iota(jnp.int32, (8, basis), 0)
            third = quarter - one - two
            out[rows : rows + 8] = power(jnp.where(at == 0, one, jnp.where(at == 1, two, third)))


def settle(terms, kept, arrived, tiles):
    rows, basis = kept.shape[1:]
    shapes = [jax.ShapeDtypeStruct((rows, basis), F32)]
    shapes += [jax.ShapeDtypeStruct((rows + 8, basis), F32)] * (SIDE - 1)
    return pl.pallas_call(
        functools.partial(settle_kernel, terms),
        out_shape=shapes,
        in_specs=[VMEM] * 8,
        out_specs=[VMEM] * SIDE,
        compiler_params=limit(8),
    )(kept, *arrived, *tiles)


def last_kernel(kept, *refs):
    arrived, outs, scratch = refs[:3], refs[3:-1], refs[-1]
    _, core, _, z = here()
    whole = kept[...]
    high = whole.shape[0]
    for block in arrived:
        rate = block[high : high + 1, 0:1] * block[high + 1 : high + 2, 0:1] * block[high + 2 : high + 3, 0:1]
        rate = rate * rate
        whole = whole + block[:high] * (rate * rate)
    rows = high // SIDE
    for v in range(SIDE):
        scratch[v] = whole[v * rows : (v + 1) * rows]
    for slot, out in zip(order_here(z, 3, core), outs):
        out[...] = scratch[slot]


def last(kept, arrived):
    rows, basis = kept.shape
    part = jax.ShapeDtypeStruct((rows // SIDE, basis), F32)
    return pl.pallas_call(
        last_kernel,
        out_shape=[part] * SIDE,
        in_specs=[VMEM] * 4,
        out_specs=[VMEM] * SIDE,
        scratch_shapes=[pltpu.VMEM((SIDE, rows // SIDE, basis), F32)],
        compiler_params=limit(4),
    )(kept, *arrived)


def go(v, *moves):
    return lax.ppermute(v, AXES, partners(*moves))


def on_device(factors, screen):
    aux, occ, basis = factors.shape
    own = factors.reshape(aux * occ, basis)
    other = lax.ppermute(own, AXES, CORE_SWAP)
    other_screen = lax.ppermute(screen, AXES, CORE_SWAP)
    depth = CORES * aux * occ

    own_high, own_low, peak = front(screen, own, aux, ((2, 3), (0, 1)), True)
    peak_other = lax.ppermute(peak, AXES, CORE_SWAP)
    (other_high,) = front(other_screen, other, aux, ((2, 3),), False)
    (other_low,) = front(other_screen, other, aux, ((0, 1),), False)
    high = (own, own_high, other, other_high)
    low = (own, own_low, other, other_low)
    peaks = (peak, peak_other)

    def narrow(v):
        return v.astype(SENT)

    def wide(v):
        return v.astype(F32)

    d_moves, y_moves, x_moves = ((0, 0), (2, 0)), ((0, 0),), ((2, 0),)
    d_out = product((*high, *peaks), ((0, 2), (0, 3), (1, 2), (1, 3)))
    d_in = go(narrow(d_out), *d_moves)
    y_out = product((*high, *peaks), ((0, 0), (0, 1), (1, 0), (1, 1)))
    y_in = go(narrow(y_out), *y_moves)
    x_out = product((*low, *peaks), ((0, 2), (0, 3), (1, 2), (1, 3)))
    x_in = go(narrow(x_out), *x_moves)
    kept = product(low, ((0, 0), (0, 1), (1, 0), (1, 1)))
    peak = jnp.maximum(jnp.maximum(peak, peak_other), SMALLEST)
    d_most = go(peak, *d_moves)
    y_most = go(peak, *y_moves)
    x_most = go(peak, *x_moves)
    kept, x_out, y_out, d_out = settle(
        depth, kept, (wide(d_in), wide(y_in), wide(x_in)), (peak, d_most, y_most, x_most)
    )

    d_moves, y_moves, x_moves = ((0, 1), (2, 1)), ((0, 1),), ((2, 1),)
    d_in = go(narrow(d_out), *d_moves)
    y_in = go(narrow(y_out), *y_moves)
    x_in = go(narrow(x_out), *x_moves)
    kept, second, first, across = last(kept, (wide(d_in), wide(y_in), wide(x_in)))
    z_across = go(across, (3, 0), (3, 1))
    z_second = go(second, (3, 1))
    z_first = go(first, (3, 0))
    return kept + z_second + z_first + z_across


def solution(mesh):
    placed = (P(AXES, None, None), P(AXES, None))
    return jax.shard_map(on_device, mesh=mesh, in_specs=placed, out_specs=P(AXES, None), check_vma=False)
```

```python
import functools

import jax
import jax.numpy as jnp
from jax import lax
from jax.experimental import pallas as pl
from jax.experimental.pallas import tpu as pltpu
from jax.sharding import PartitionSpec as P


AXES = ("grp", "mem")
SIDE = 4
CORES = 2
SENT = jnp.float16
ROOM = 16384.0
SMALLEST = 2.0**-60
F32 = jnp.float32


def limit(mib):
    return pltpu.CompilerParams(vmem_limit_bytes=mib * 1024 * 1024)


VMEM = pl.BlockSpec(memory_space=pltpu.VMEM)
SMEM = pl.BlockSpec(memory_space=pltpu.SMEM)


def near(v):
    return v ^ 1


def far(v):
    return SIDE - 1 - v


def steps(dim, core):
    return (near, far) if core == (dim == 2) else (far, near)


def linear(y, c, x, z):
    return ((y * CORES + c) * SIDE + x) * SIDE + z


def everyone():
    return [(y, c, x, z) for y in range(SIDE) for c in range(CORES) for x in range(SIDE) for z in range(SIDE)]


def partners(*moves):
    pairs = []
    for place in everyone():
        target = list(place)
        for dim, turn in moves:
            target[dim] = steps(dim, place[1])[turn](target[dim])
        pairs.append((linear(*place), linear(*target)))
    return pairs


CORE_SWAP = [(linear(y, c, x, z), linear(y, 1 - c, x, z)) for y, c, x, z in everyone()]


def here():
    group, member = lax.axis_index("grp"), lax.axis_index("mem")
    return lax.div(group, CORES), lax.rem(group, CORES), lax.div(member, SIDE), lax.rem(member, SIDE)


def order_here(v, dim, core):
    near_first = core == int(dim == 2)
    close, distant = v ^ 1, SIDE - 1 - v
    first, second = jnp.where(near_first, close, distant), jnp.where(near_first, distant, close)
    return [v, second, first, v ^ 2]


def bound(most, terms):
    return terms * most * most


def padded(size, tile):
    return -(-size // tile) * tile


def front_kernel(slots, aux, screen, x_ref, *refs):
    outs, scratch = refs[:-1], refs[-1]
    y, core, x, z = here()
    depth, basis = x_ref.shape
    blocks = screen.shape[1]
    part = basis // (SIDE * CORES)
    chunk = part // SIDE
    span = scratch.shape[1]
    occ = depth // aux
    lane = lax.broadcasted_iota(jnp.int32, (16, depth), 1)
    block_of = lax.div(lax.rem(lane, occ), occ // blocks)
    flags = jnp.zeros((16, depth), F32)
    for b in range(blocks):
        flags = jnp.where(block_of == b, (screen[0, b] == 1).astype(F32), flags)
    flags = flags.astype(x_ref.dtype)
    if len(outs) > len(slots):
        width = occ // blocks
        most = jnp.zeros((width, basis), F32)
        for r in range(0, depth, width):
            kept = (screen[0, (r % occ) // width] == 1).astype(F32)
            most = jnp.maximum(most, jnp.abs(x_ref[r : r + width, :]).astype(F32) * kept)
        top = jnp.max(jnp.max(most, axis=1, keepdims=True), axis=0, keepdims=True)
        spread = 1.0 + 0.4 * ((y * SIDE + x) * SIDE + z).astype(F32) / SIDE**3
        outs[-1][...] = jnp.broadcast_to(top * spread, outs[-1].shape)
    places = order_here(y, 0, core)
    for n, pair in enumerate(slots):
        for s, slot in enumerate(pair):
            start = (places[slot] * CORES + core) * part
            tile = jnp.minimum(lax.div(start, 128), (basis - span) // 128)
            held = scratch.at[(2 * n + s) % 2]
            held[...] = x_ref[:, pl.ds(pl.multiple_of(tile * 128, 128), span)].T
            block = held[pl.ds(pl.multiple_of(start - tile * 128, 16), part), :] * flags[0:1]
            for v in range(SIDE):
                outs[n][s, v] = block[v * chunk : (v + 1) * chunk]


def front(screen, x, aux, slots, peak):
    depth, basis = x.shape
    part = basis // (SIDE * CORES)
    span = padded(part + 127, 128)
    shapes = [jax.ShapeDtypeStruct((2, SIDE, part // SIDE, depth), x.dtype)] * len(slots)
    if peak:
        shapes.append(jax.ShapeDtypeStruct((8, 128), F32))
    return pl.pallas_call(
        functools.partial(front_kernel, slots, aux),
        out_shape=shapes,
        in_specs=[SMEM, VMEM],
        out_specs=[VMEM] * len(shapes),
        scratch_shapes=[pltpu.VMEM((2, span, depth), x.dtype)],
        compiler_params=limit(12),
    )(screen, x)


def bound(most, terms):
    return terms * most * most


def product_kernel(slots, x_own, t_own, x_other, t_other, *refs):
    out = refs[-1]
    _, core, x, _ = here()
    x_order = order_here(x, 2, core)
    chunk = t_own.shape[2]

    def left(x_t):
        return jnp.concatenate([x_t[i, x_order[j]] for i, j in slots], axis=0)

    whole = jnp.dot(left(t_own), x_own[...], preferred_element_type=F32)
    whole = whole + jnp.dot(left(t_other), x_other[...], preferred_element_type=F32)
    if len(refs) > 1:
        most = jnp.maximum(jnp.maximum(refs[0][0:1, 0:1], refs[1][0:1, 0:1]), SMALLEST)
        whole = whole * (ROOM / bound(most, CORES * x_own.shape[0]))
    for at in range(len(slots)):
        out[at] = whole[at * chunk : (at + 1) * chunk]


def product(parts, slots):
    chunk, depth = parts[1].shape[2:]
    basis = parts[0].shape[1]
    rows = len(slots) * chunk
    return pl.pallas_call(
        functools.partial(product_kernel, slots),
        out_shape=jax.ShapeDtypeStruct((len(slots), chunk, basis), F32),
        in_specs=[VMEM] * len(parts),
        out_specs=VMEM,
        compiler_params=limit(16),
        cost_estimate=pl.CostEstimate(flops=4 * rows * depth * basis, bytes_accessed=4 * rows * basis, transcendentals=0),
    )(*parts)


def power(e):
    return jnp.exp2(e).astype(jnp.bfloat16).astype(F32)


def settle_kernel(terms, kept, *refs):
    arrived, tiles, outs = refs[:3], refs[3:7], refs[7:]
    most = tiles[0][0:1, 0:1]
    rates = []
    for tile in tiles[1:]:
        most = jnp.maximum(most, tile[0:1, 0:1])
        rates.append(bound(tile[0:1, 0:1], terms) / ROOM)
    quarter = jnp.ceil(jnp.log2(bound(most, SIDE * terms) / ROOM) * 0.25)
    one = jnp.floor(quarter / 3)
    two = jnp.floor((quarter - one) / 2)
    y, _, x, _ = here()
    spread = 1.0 + (y * SIDE + x).astype(F32) / SIDE**2
    scale = power(-4 * quarter) / (spread * spread * spread * spread)
    rows, basis = kept.shape[1:]
    for slot, out in enumerate(outs):
        whole = kept[slot]
        for block, rate in zip(arrived, rates):
            whole = whole + block[slot] * rate
        out[:rows] = whole * scale if slot else whole
        if slot:
            at = lax.broadcasted_iota(jnp.int32, (8, basis), 0)
            third = power(quarter - one - two) * spread
            out[rows : rows + 8] = jnp.where(at == 0, power(one), jnp.where(at == 1, power(two), third))


def settle(terms, kept, arrived, tiles):
    rows, basis = kept.shape[1:]
    shapes = [jax.ShapeDtypeStruct((rows, basis), F32)]
    shapes += [jax.ShapeDtypeStruct((rows + 8, basis), F32)] * (SIDE - 1)
    return pl.pallas_call(
        functools.partial(settle_kernel, terms),
        out_shape=shapes,
        in_specs=[VMEM] * 8,
        out_specs=[VMEM] * SIDE,
        compiler_params=limit(8),
    )(kept, *arrived, *tiles)


def last_kernel(kept, *refs):
    arrived, outs, scratch = refs[:3], refs[3:-1], refs[-1]
    _, core, _, z = here()
    whole = kept[...]
    high = whole.shape[0]
    for block in arrived:
        rate = block[high : high + 1, 0:1] * block[high + 1 : high + 2, 0:1] * block[high + 2 : high + 3, 0:1]
        rate = rate * rate
        whole = whole + block[:high] * (rate * rate)
    rows = high // SIDE
    for v in range(SIDE):
        scratch[v] = whole[v * rows : (v + 1) * rows]
    for slot, out in zip(order_here(z, 3, core), outs):
        out[...] = scratch[slot]


def last(kept, arrived):
    rows, basis = kept.shape
    part = jax.ShapeDtypeStruct((rows // SIDE, basis), F32)
    return pl.pallas_call(
        last_kernel,
        out_shape=[part] * SIDE,
        in_specs=[VMEM] * 4,
        out_specs=[VMEM] * SIDE,
        scratch_shapes=[pltpu.VMEM((SIDE, rows // SIDE, basis), F32)],
        compiler_params=limit(4),
    )(kept, *arrived)


def go(v, *moves):
    return lax.ppermute(v, AXES, partners(*moves))


def on_device(factors, screen):
    aux, occ, basis = factors.shape
    own = factors.reshape(aux * occ, basis)
    other = lax.ppermute(own, AXES, CORE_SWAP)
    other_screen = lax.ppermute(screen, AXES, CORE_SWAP)
    depth = CORES * aux * occ

    own_high, own_low, peak = front(screen, own, aux, ((2, 3), (0, 1)), True)
    peak_other = lax.ppermute(peak, AXES, CORE_SWAP)
    (other_high,) = front(other_screen, other, aux, ((2, 3),), False)
    (other_low,) = front(other_screen, other, aux, ((0, 1),), False)
    high = (own, own_high, other, other_high)
    low = (own, own_low, other, other_low)
    peaks = (peak, peak_other)

    def narrow(v):
        return v.astype(SENT)

    def wide(v):
        return v.astype(F32)

    d_moves, y_moves, x_moves = ((0, 0), (2, 0)), ((0, 0),), ((2, 0),)
    d_out = product((*high, *peaks), ((0, 2), (0, 3), (1, 2), (1, 3)))
    d_in = go(narrow(d_out), *d_moves)
    y_out = product((*high, *peaks), ((0, 0), (0, 1), (1, 0), (1, 1)))
    y_in = go(narrow(y_out), *y_moves)
    x_out = product((*low, *peaks), ((0, 2), (0, 3), (1, 2), (1, 3)))
    x_in = go(narrow(x_out), *x_moves)
    kept = product(low, ((0, 0), (0, 1), (1, 0), (1, 1)))
    peak = jnp.maximum(jnp.maximum(peak, peak_other), SMALLEST)
    d_most = go(peak, *d_moves)
    y_most = go(peak, *y_moves)
    x_most = go(peak, *x_moves)
    kept, x_out, y_out, d_out = settle(
        depth, kept, (wide(d_in), wide(y_in), wide(x_in)), (peak, d_most, y_most, x_most)
    )

    d_moves, y_moves, x_moves = ((0, 1), (2, 1)), ((0, 1),), ((2, 1),)
    d_in = go(narrow(d_out), *d_moves)
    y_in = go(narrow(y_out), *y_moves)
    x_in = go(narrow(x_out), *x_moves)
    kept, second, first, across = last(kept, (wide(d_in), wide(y_in), wide(x_in)))
    z_across = go(across, (3, 0), (3, 1))
    z_second = go(second, (3, 1))
    z_first = go(first, (3, 0))
    return kept + z_second + z_first + z_across


def solution(mesh):
    placed = (P(AXES, None, None), P(AXES, None))
    return jax.shard_map(on_device, mesh=mesh, in_specs=placed, out_specs=P(AXES, None), check_vma=False)
```

```python
import functools

import jax
import jax.numpy as jnp
from jax import lax
from jax.experimental import pallas as pl
from jax.experimental.pallas import tpu as pltpu
from jax.sharding import PartitionSpec as P


AXES = ("grp", "mem")
SIDE = 4
CORES = 2
SENT = jnp.float16
ROOM = 16384.0
SMALLEST = 2.0**-60
F32 = jnp.float32


def limit(mib):
    return pltpu.CompilerParams(vmem_limit_bytes=mib * 1024 * 1024)


VMEM = pl.BlockSpec(memory_space=pltpu.VMEM)
SMEM = pl.BlockSpec(memory_space=pltpu.SMEM)


def near(v):
    return v ^ 1


def far(v):
    return SIDE - 1 - v


def steps(dim, core):
    return (near, far) if core == (dim == 2) else (far, near)


def linear(y, c, x, z):
    return ((y * CORES + c) * SIDE + x) * SIDE + z


def everyone():
    return [(y, c, x, z) for y in range(SIDE) for c in range(CORES) for x in range(SIDE) for z in range(SIDE)]


def partners(*moves):
    pairs = []
    for place in everyone():
        target = list(place)
        for dim, turn in moves:
            target[dim] = steps(dim, place[1])[turn](target[dim])
        pairs.append((linear(*place), linear(*target)))
    return pairs


CORE_SWAP = [(linear(y, c, x, z), linear(y, 1 - c, x, z)) for y, c, x, z in everyone()]


def here():
    group, member = lax.axis_index("grp"), lax.axis_index("mem")
    return lax.div(group, CORES), lax.rem(group, CORES), lax.div(member, SIDE), lax.rem(member, SIDE)


def order_here(v, dim, core):
    near_first = core == int(dim == 2)
    close, distant = v ^ 1, SIDE - 1 - v
    first, second = jnp.where(near_first, close, distant), jnp.where(near_first, distant, close)
    return [v, second, first, v ^ 2]


def bound(most, terms):
    return terms * most * most


def padded(size, tile):
    return -(-size // tile) * tile


def front_kernel(slots, aux, screen, x_ref, *refs):
    outs, scratch = refs[:-1], refs[-1]
    y, core, x, z = here()
    depth, basis = x_ref.shape
    blocks = screen.shape[1]
    part = basis // (SIDE * CORES)
    chunk = part // SIDE
    span = scratch.shape[1]
    occ = depth // aux
    lane = lax.broadcasted_iota(jnp.int32, (16, depth), 1)
    block_of = lax.div(lax.rem(lane, occ), occ // blocks)
    flags = jnp.zeros((16, depth), F32)
    for b in range(blocks):
        flags = jnp.where(block_of == b, (screen[0, b] == 1).astype(F32), flags)
    flags = flags.astype(x_ref.dtype)
    if len(outs) > len(slots):
        width = occ // blocks
        most = jnp.zeros((width, basis), F32)
        for r in range(0, depth, width):
            kept = (screen[0, (r % occ) // width] == 1).astype(F32)
            most = jnp.maximum(most, jnp.abs(x_ref[r : r + width, :]).astype(F32) * kept)
        top = jnp.max(jnp.max(most, axis=1, keepdims=True), axis=0, keepdims=True)
        spread = 1.0 + 0.4 * ((y * SIDE + x) * SIDE + z).astype(F32) / SIDE**3
        outs[-1][...] = jnp.broadcast_to(top * spread, outs[-1].shape)
    places = order_here(y, 0, core)
    for n, pair in enumerate(slots):
        for s, slot in enumerate(pair):
            start = (places[slot] * CORES + core) * part
            tile = jnp.minimum(lax.div(start, 128), (basis - span) // 128)
            held = scratch.at[(2 * n + s) % 2]
            held[...] = x_ref[:, pl.ds(pl.multiple_of(tile * 128, 128), span)].T
            block = held[pl.ds(pl.multiple_of(start - tile * 128, 16), part), :] * flags[0:1]
            for v in range(SIDE):
                outs[n][s, v] = block[v * chunk : (v + 1) * chunk]


def front(screen, x, aux, slots, peak):
    depth, basis = x.shape
    part = basis // (SIDE * CORES)
    span = padded(part + 127, 128)
    shapes = [jax.ShapeDtypeStruct((2, SIDE, part // SIDE, depth), x.dtype)] * len(slots)
    if peak:
        shapes.append(jax.ShapeDtypeStruct((8, 128), F32))
    return pl.pallas_call(
        functools.partial(front_kernel, slots, aux),
        out_shape=shapes,
        in_specs=[SMEM, VMEM],
        out_specs=[VMEM] * len(shapes),
        scratch_shapes=[pltpu.VMEM((2, span, depth), x.dtype)],
        compiler_params=limit(12),
    )(screen, x)


def bound(most, terms):
    return terms * most * most


def product_kernel(slots, x_own, t_own, x_other, t_other, *refs):
    out = refs[-1]
    _, core, x, _ = here()
    x_order = order_here(x, 2, core)
    chunk = t_own.shape[2]

    def left(x_t):
        return jnp.concatenate([x_t[i, x_order[j]] for i, j in slots], axis=0)

    whole = jnp.dot(left(t_own), x_own[...], preferred_element_type=F32)
    whole = whole + jnp.dot(left(t_other), x_other[...], preferred_element_type=F32)
    if len(refs) > 1:
        most = jnp.maximum(jnp.maximum(refs[0][0:1, 0:1], refs[1][0:1, 0:1]), SMALLEST)
        whole = whole * (ROOM / bound(most, CORES * x_own.shape[0]))
    for at in range(len(slots)):
        out[at] = whole[at * chunk : (at + 1) * chunk]


def product(parts, slots):
    chunk, depth = parts[1].shape[2:]
    basis = parts[0].shape[1]
    rows = len(slots) * chunk
    return pl.pallas_call(
        functools.partial(product_kernel, slots),
        out_shape=jax.ShapeDtypeStruct((len(slots), chunk, basis), F32),
        in_specs=[VMEM] * len(parts),
        out_specs=VMEM,
        compiler_params=limit(16),
        cost_estimate=pl.CostEstimate(flops=4 * rows * depth * basis, bytes_accessed=4 * rows * basis, transcendentals=0),
    )(*parts)


def power(e):
    return jnp.exp2(e).astype(jnp.bfloat16).astype(F32)


def settle_kernel(slots, terms, kept, *refs):
    arrived, tiles, outs = refs[:3], refs[3:7], refs[7:]
    most = tiles[0][0:1, 0:1]
    rates = []
    for tile in tiles[1:]:
        most = jnp.maximum(most, tile[0:1, 0:1])
        rates.append(bound(tile[0:1, 0:1], terms) / ROOM)
    quarter = jnp.ceil(jnp.log2(bound(most, SIDE * terms) / ROOM) * 0.25)
    one = jnp.floor(quarter / 3)
    two = jnp.floor((quarter - one) / 2)
    y, _, x, _ = here()
    spread = 1.0 + (y * SIDE + x).astype(F32) / SIDE**2
    scale = power(-4 * quarter) / (spread * spread * spread * spread)
    rows, basis = kept.shape[1:]
    for slot, out in zip(slots, outs):
        whole = kept[slot]
        for block, rate in zip(arrived, rates):
            whole = whole + block[slot] * rate
        out[:rows] = whole * scale if slot else whole
        if slot:
            at = lax.broadcasted_iota(jnp.int32, (8, basis), 0)
            third = power(quarter - one - two) * spread
            out[rows : rows + 8] = jnp.where(at == 0, power(one), jnp.where(at == 1, power(two), third))


def settle(slots, terms, kept, arrived, tiles):
    rows, basis = kept.shape[1:]
    shapes = [jax.ShapeDtypeStruct((rows + 8 if slot else rows, basis), F32) for slot in slots]
    return pl.pallas_call(
        functools.partial(settle_kernel, slots, terms),
        out_shape=shapes,
        in_specs=[VMEM] * 8,
        out_specs=[VMEM] * len(slots),
        compiler_params=limit(8),
    )(kept, *arrived, *tiles)


def last_kernel(kept, *refs):
    arrived, outs, scratch = refs[:3], refs[3:-1], refs[-1]
    _, core, _, z = here()
    whole = kept[...]
    high = whole.shape[0]
    for block in arrived:
        rate = block[high : high + 1, 0:1] * block[high + 1 : high + 2, 0:1] * block[high + 2 : high + 3, 0:1]
        rate = rate * rate
        whole = whole + block[:high] * (rate * rate)
    rows = high // SIDE
    for v in range(SIDE):
        scratch[v] = whole[v * rows : (v + 1) * rows]
    for slot, out in zip(order_here(z, 3, core), outs):
        out[...] = scratch[slot]


def last(kept, arrived):
    rows, basis = kept.shape
    part = jax.ShapeDtypeStruct((rows // SIDE, basis), F32)
    return pl.pallas_call(
        last_kernel,
        out_shape=[part] * SIDE,
        in_specs=[VMEM] * 4,
        out_specs=[VMEM] * SIDE,
        scratch_shapes=[pltpu.VMEM((SIDE, rows // SIDE, basis), F32)],
        compiler_params=limit(4),
    )(kept, *arrived)


def go(v, *moves):
    return lax.ppermute(v, AXES, partners(*moves))


def on_device(factors, screen):
    aux, occ, basis = factors.shape
    own = factors.reshape(aux * occ, basis)
    other = lax.ppermute(own, AXES, CORE_SWAP)
    other_screen = lax.ppermute(screen, AXES, CORE_SWAP)
    depth = CORES * aux * occ

    own_high, own_low, peak = front(screen, own, aux, ((2, 3), (0, 1)), True)
    peak_other = lax.ppermute(peak, AXES, CORE_SWAP)
    (other_high,) = front(other_screen, other, aux, ((2, 3),), False)
    (other_low,) = front(other_screen, other, aux, ((0, 1),), False)
    high = (own, own_high, other, other_high)
    low = (own, own_low, other, other_low)
    peaks = (peak, peak_other)

    def narrow(v):
        return v.astype(SENT)

    def wide(v):
        return v.astype(F32)

    d_moves, y_moves, x_moves = ((0, 0), (2, 0)), ((0, 0),), ((2, 0),)
    d_out = product((*high, *peaks), ((0, 2), (0, 3), (1, 2), (1, 3)))
    d_in = go(narrow(d_out), *d_moves)
    y_out = product((*high, *peaks), ((0, 0), (0, 1), (1, 0), (1, 1)))
    y_in = go(narrow(y_out), *y_moves)
    x_out = product((*low, *peaks), ((0, 2), (0, 3), (1, 2), (1, 3)))
    x_in = go(narrow(x_out), *x_moves)
    kept = product(low, ((0, 0), (0, 1), (1, 0), (1, 1)))
    peak = jnp.maximum(jnp.maximum(peak, peak_other), SMALLEST)
    d_most = go(peak, *d_moves)
    y_most = go(peak, *y_moves)
    x_most = go(peak, *x_moves)
    first_round = (depth, kept, (wide(d_in), wide(y_in), wide(x_in)), (peak, d_most, y_most, x_most))
    x_out, y_out, d_out = settle((1, 2, 3), *first_round)
    (kept,) = settle((0,), *first_round)

    d_moves, y_moves, x_moves = ((0, 1), (2, 1)), ((0, 1),), ((2, 1),)
    d_in = go(narrow(d_out), *d_moves)
    y_in = go(narrow(y_out), *y_moves)
    x_in = go(narrow(x_out), *x_moves)
    kept, second, first, across = last(kept, (wide(d_in), wide(y_in), wide(x_in)))
    z_across = go(across, (3, 0), (3, 1))
    z_second = go(second, (3, 1))
    z_first = go(first, (3, 0))
    return kept + z_second + z_first + z_across


def solution(mesh):
    placed = (P(AXES, None, None), P(AXES, None))
    return jax.shard_map(on_device, mesh=mesh, in_specs=placed, out_specs=P(AXES, None), check_vma=False)
```
